32 devices in a mesh: grp: 1, sp: 32 (over z, y, x, core), ch: 1.
Axes of the slice: x: 2, y: 2, z: 4, core: 2. Of those that a mesh axis runs over, the one named last changes fastest.
Arguments:
- latents: bfloat16 [131072, 1024], P(('grp', 'sp')), may hold values from -6 to 6
- spectrum: bfloat16 [16, 64, 128, 1024], P(None, None, 'sp', 'ch'), may hold values from -4 to 4
- w_value: bfloat16 [1024, 1024], P('sp', 'ch'), may hold values from -0.1875 to 0.1875
- w_gate: bfloat16 [1024, 1024], P('sp', 'ch'), may hold values from -0.1875 to 0.1875
- w_out: bfloat16 [1024, 1024], P('sp'), may hold values from -0.1875 to 0.1875
- embed_table: bfloat16 [1024, 32768], P(('sp', 'ch')), may hold values from -12 to 12
- prompt_ids: int32 [256], P('grp'), may hold values from 0 to 32767
- noise_step: int32 [1], P('grp'), may hold values from 0 to 999
Outputs:
- denoised: bfloat16 [131072, 1024], P(('grp', 'sp', 'ch'))
The draws below stay inside these ranges and needn't reach their ends.
All inputs are finite; a program needn't handle non-finite values.
Results may differ from the reference program's by a relative error of at most 0.013.
Values may be sent and summed in bfloat16 or wider, within the bound.
A program may use at most 128 MiB of HBM per device.

```python
import math
import jax
import jax.numpy as jnp
import numpy as np
from jax import lax

TT = 16
HH = 64
WW = 128
C = 1024
VOCAB = 32768
PROMPT = 256
CELLS = 131072


def plant(drawn, own_key, low, high):
    longest = drawn.shape.index(max(drawn.shape))
    spots = []
    for shift in (0, 1):
        where = [jax.random.randint(jax.random.fold_in(own_key, axis), (), 0, length) for axis, length in enumerate(drawn.shape)]
        where[longest] = (where[longest] + shift) % drawn.shape[longest]
        spots.append(tuple(where))
    return drawn.at[spots[0]].set(low).at[spots[1]].set(high)


def shard_levels(key, dims, cuts, least, top_value):
    loudness, own = 1.0, jax.random.fold_in(key, 6)
    for axis_at, shards_of in cuts:
        draws = jnp.exp(jax.random.uniform(jax.random.fold_in(own, axis_at), (shards_of,), jnp.float32, least / len(cuts), top_value / len(cuts)))
        loudness = loudness * jnp.repeat(draws, dims[axis_at] // shards_of).reshape([-1 if axis == axis_at else 1 for axis in range(len(dims))])
    return loudness


def rank_table(amount, slope):
    weights = [(1 << 20) // math.isqrt(grade ** slope) + 1 for grade in range(1, amount + 1)]
    width = 1 + sum(weights) // (1 << 30)
    return np.cumsum(np.array([max(1, weight // width) for weight in weights]))


def ranked(key, dims, count, lean):
    table = rank_table(count, lean)
    lot = jax.random.randint(jax.random.fold_in(key, 1), dims, 0, int(table[count - 1]))
    rank = jnp.searchsorted(jnp.asarray(table, jnp.int32), lot, side="right")
    return jax.random.permutation(jax.random.fold_in(key, 2), count)[rank].astype(jnp.int32)


def bell_draw(own_key, dims, scale, limit, cuts=(), held_as=jnp.bfloat16):
    values = scale * jax.random.normal(own_key, dims, jnp.float32)
    if cuts:
        values = values * shard_levels(own_key, dims, cuts, -0.22, 0.18)
    return jnp.clip(values, -limit, limit).astype(held_as)


def setup_inputs(seed: int = 0, part: int = 0) -> dict:
    key_list = jax.random.split(jax.random.key(seed), 9)
    part_keys = jax.random.split(jax.random.fold_in(key_list[8], part), 9)
    latents = bell_draw(part_keys[0], (CELLS, C), 1.0, 6.0, ((0, 32),))
    spectrum = bell_draw(key_list[1], (TT, HH, WW, C), 1.0, 4.0, ((2, 32),))
    w_value = bell_draw(key_list[2], (C, C), C ** -0.5, 0.1875, ((0, 32),))
    w_gate = bell_draw(key_list[3], (C, C), C ** -0.5, 0.1875, ((0, 32),))
    w_out = bell_draw(key_list[4], (C, C), C ** -0.5, 0.1875, ((0, 32),))
    embed_table = bell_draw(key_list[5], (C, VOCAB), 3.0, 12.0, ((0, 32),))
    prompt_ids = plant(ranked(part_keys[6], (PROMPT,), VOCAB, 2), jax.random.fold_in(part_keys[6], 3), 0, VOCAB - 1).astype(jnp.int32)
    noise_step = jax.random.randint(part_keys[7], (1,), 0, 1000).astype(jnp.int32)
    return {"latents": latents, "spectrum": spectrum, "w_value": w_value, "w_gate": w_gate, "w_out": w_out, "embed_table": embed_table, "prompt_ids": prompt_ids, "noise_step": noise_step}


def cas_table(length):
    position = jnp.arange(length, dtype=jnp.int32)
    product = position[:, None] * position[None, :] % length
    phase_angle = product.astype(jnp.float32) * (2.0 * math.pi / length)
    return ((jnp.cos(phase_angle) + jnp.sin(phase_angle)) / math.sqrt(length)).astype(jnp.bfloat16)

def step_embedding(noise_step, channel, channels):
    half_count = channels // 2
    lower_half = channel < half_count
    position = jnp.where(lower_half, channel, channel - half_count).astype(jnp.float32)
    frequency = jnp.exp(-math.log(10000.0) * position / half_count)
    phase_angle = noise_step[0].astype(jnp.float32) * frequency
    return jnp.where(lower_half, jnp.sin(phase_angle), jnp.cos(phase_angle))

def apply_table(form, table, operand):
    return jnp.einsum(form, table.astype(jnp.float32), operand.astype(jnp.float32), precision=lax.Precision.HIGHEST)

def reference(latents, spectrum, w_value, w_gate, w_out, embed_table, prompt_ids, noise_step):
    channel = jnp.arange(C, dtype=jnp.int32)
    pooled = lax.optimization_barrier(jnp.mean(jnp.take(embed_table, prompt_ids, axis=1).astype(jnp.float32), axis=1))
    modulation = 1.0 + pooled + step_embedding(noise_step, channel, C)
    value_rows = jnp.dot(latents, w_value, preferred_element_type=jnp.float32).astype(jnp.bfloat16)
    gate_rows = jnp.dot(latents, w_gate, preferred_element_type=jnp.float32)
    cas_width = cas_table(WW)
    cas_height = cas_table(HH)
    cas_time = cas_table(TT)
    latent_grid = value_rows.reshape(TT, HH, WW, C)
    width_spec = apply_table('kw,thwc->thkc', cas_width, latent_grid).astype(jnp.bfloat16)
    height_spec = apply_table('ah,thkc->takc', cas_height, width_spec).astype(jnp.bfloat16)
    full_spec = apply_table('st,takc->sakc', cas_time, height_spec).astype(jnp.bfloat16)
    filtered = (full_spec.astype(jnp.float32) * spectrum.astype(jnp.float32)).astype(jnp.bfloat16)
    time_back = apply_table('ts,sakc->takc', cas_time, filtered).astype(jnp.bfloat16)
    height_back = apply_table('ha,takc->thkc', cas_height, time_back).astype(jnp.bfloat16)
    mix_rows = apply_table('wk,thkc->thwc', cas_width, height_back).reshape(TT * HH * WW, C)
    mixed_rows = (mix_rows * jax.nn.silu(gate_rows) * modulation[None, :]).astype(jnp.bfloat16)
    projected = jnp.dot(mixed_rows, w_out, preferred_element_type=jnp.float32)
    return (latents.astype(jnp.float32) + projected).astype(jnp.bfloat16)
```

```python
import math

import jax
import jax.numpy as jnp
from jax import lax
from jax.experimental import pallas as pl
from jax.experimental.pallas import tpu as pltpu
from jax.sharding import PartitionSpec as P

TT = 16
HH = 64
WW = 128
C = 1024

TILE = 16


def cas_table(length):
    position = jnp.arange(length, dtype=jnp.int32)
    product = position[:, None] * position[None, :] % length
    phase_angle = product.astype(jnp.float32) * (2.0 * math.pi / length)
    return ((jnp.cos(phase_angle) + jnp.sin(phase_angle)) / math.sqrt(length)).astype(jnp.bfloat16)


def step_embedding(noise_step, channel, channels):
    half_count = channels // 2
    lower_half = channel < half_count
    position = jnp.where(lower_half, channel, channel - half_count).astype(jnp.float32)
    frequency = jnp.exp(-math.log(10000.0) * position / half_count)
    phase_angle = noise_step[0].astype(jnp.float32) * frequency
    return jnp.where(lower_half, jnp.sin(phase_angle), jnp.cos(phase_angle))


def widened(table, copies):
    length = table.shape[0]
    inner = jnp.eye(copies, dtype=table.dtype)
    both = table[:, None, :, None] * inner[None, :, None, :]
    return both.reshape(length * copies, length * copies)


def dot(left, right):
    return jnp.dot(left, right, preferred_element_type=jnp.float32)


def width_kernel(table_ref, latents_ref, out_ref):
    owners, rows, channels = out_ref.shape
    moved = dot(table_ref[...], latents_ref[...])
    out_ref[...] = moved.reshape(owners, rows, channels).astype(out_ref.dtype)


def width_forward(table, latents, owners, lines, band, group):
    channels = latents.shape[1]
    rows = group * WW
    cells = lines * WW
    return pl.pallas_call(
        width_kernel,
        grid=(lines // group,),
        in_specs=[
            pl.BlockSpec(table.shape, lambda g: (0, 0)),
            pl.BlockSpec((rows, channels), lambda g: (g, 0)),
        ],
        out_specs=pl.BlockSpec((owners, group * band, channels), lambda g: (0, g, 0)),
        out_shape=jax.ShapeDtypeStruct((owners, lines * band, channels), jnp.bfloat16),
        compiler_params=pltpu.CompilerParams(vmem_limit_bytes=48 * 2**20),
        cost_estimate=pl.CostEstimate(
            flops=2 * cells * table.shape[0] * channels,
            bytes_accessed=4 * cells * channels,
            transcendentals=0,
        ),
        name="width_forward",
    )(table, latents)


def plane_kernel(band, height_ref, time_ref, planes_ref, weight_ref, spectrum_ref, out_ref, spec):
    per_frame = HH * band
    width = out_ref.shape[1]
    pieces = per_frame // TILE
    weight = weight_ref[...].reshape(planes_ref.shape[1], width)

    def forward(t, carry):
        rows = pl.ds(pl.multiple_of(t * per_frame, per_frame), per_frame)
        value = dot(planes_ref[rows, :], weight).astype(jnp.bfloat16)
        spec[t] = dot(height_ref[...], value).astype(jnp.bfloat16)
        return carry

    lax.fori_loop(0, TT, forward, 0, unroll=4)

    def across(p, carry):
        rows = pl.ds(pl.multiple_of(p * TILE, TILE), TILE)
        block = spec[:, rows, :].reshape(TT * TILE, width)
        full = dot(time_ref[...], block)
        gain = spectrum_ref[:, rows, :].reshape(TT * TILE, width).astype(jnp.float32)
        filtered = (full * gain).astype(jnp.bfloat16)
        back = dot(time_ref[...], filtered).astype(jnp.bfloat16)
        spec[:, rows, :] = back.reshape(TT, TILE, width)
        return carry

    lax.fori_loop(0, pieces, across, 0, unroll=4)

    def backward(t, carry):
        rows = pl.ds(pl.multiple_of(t * per_frame, per_frame), per_frame)
        out_ref[rows, :] = dot(height_ref[...], spec[t]).astype(jnp.bfloat16)
        return carry

    lax.fori_loop(0, TT, backward, 0, unroll=4)


def plane_filter(height, time, planes, weight, spectrum, band):
    cells, channels = planes.shape
    shards, depth, chan_part = weight.shape
    width = min(256, chan_part)
    per_frame = HH * band
    return pl.pallas_call(
        lambda *refs: plane_kernel(band, *refs),
        grid=(chan_part // width,),
        in_specs=[
            pl.BlockSpec(height.shape, lambda g: (0, 0)),
            pl.BlockSpec(time.shape, lambda g: (0, 0)),
            pl.BlockSpec((cells, channels), lambda g: (0, 0)),
            pl.BlockSpec((shards, depth, width), lambda g: (0, 0, g)),
            pl.BlockSpec((TT, per_frame, width), lambda g: (0, 0, g)),
        ],
        out_specs=pl.BlockSpec((cells, width), lambda g: (0, g)),
        out_shape=jax.ShapeDtypeStruct((cells, chan_part), jnp.bfloat16),
        scratch_shapes=[pltpu.VMEM((TT, per_frame, width), jnp.bfloat16)],
        cost_estimate=pl.CostEstimate(
            flops=2 * cells * chan_part * (channels + 1024),
            bytes_accessed=2 * cells * (channels + 2 * chan_part),
            transcendentals=0,
        ),
        compiler_params=pltpu.CompilerParams(vmem_limit_bytes=56 * 2**20),
        name="plane_filter",
    )(height, time, planes, weight, spectrum)


def gate_kernel(latents_ref, gate_ref, scale_ref, out_ref):
    gate = dot(latents_ref[...], gate_ref[...].reshape(latents_ref.shape[1], out_ref.shape[1]))
    gate = gate / (1.0 + jnp.exp(-gate))
    out_ref[...] = (gate * scale_ref[...]).astype(out_ref.dtype)


def gate_rows(latents, gate_w, scale):
    cells, channels = latents.shape
    chan_part = gate_w.shape[2]
    rows = min(512, cells)
    return pl.pallas_call(
        gate_kernel,
        grid=(cells // rows,),
        in_specs=[
            pl.BlockSpec((rows, channels), lambda g: (g, 0)),
            pl.BlockSpec(gate_w.shape, lambda g: (0, 0, 0)),
            pl.BlockSpec((1, chan_part), lambda g: (0, 0)),
        ],
        out_specs=pl.BlockSpec((rows, chan_part), lambda g: (g, 0)),
        out_shape=jax.ShapeDtypeStruct((cells, chan_part), jnp.bfloat16),
        compiler_params=pltpu.CompilerParams(vmem_limit_bytes=48 * 2**20),
        cost_estimate=pl.CostEstimate(
            flops=2 * cells * channels * chan_part,
            bytes_accessed=2 * cells * (channels + chan_part),
            transcendentals=cells * chan_part,
        ),
        name="gate_rows",
    )(latents, gate_w, scale)


def mix_kernel(parts, residual, *refs):
    tables, backs = refs[:parts], refs[parts : 2 * parts]
    latents_ref, gate_ref, out_w_ref, out_ref = refs[2 * parts :]
    owners, rows, chan_part = backs[0].shape
    mix = dot(tables[0][...], backs[0][...].reshape(owners * rows, chan_part))
    for table_ref, back_ref in zip(tables[1:], backs[1:]):
        mix += dot(table_ref[...], back_ref[...].reshape(owners * rows, chan_part))
    mixed = (mix * gate_ref[...].astype(jnp.float32)).astype(jnp.bfloat16)
    projected = dot(mixed, out_w_ref[...].reshape(chan_part, out_ref.shape[1]))
    if residual:
        projected = latents_ref[...].astype(jnp.float32) + projected
    out_ref[...] = projected.astype(out_ref.dtype)


def mix_and_project(tables, backs, latents, gate, out_w, out_depth, group, residual):
    parts = len(backs)
    owners, rows_all, chan_part = backs[0].shape
    cells, channels = latents.shape
    groups = cells // (group * WW)
    rows = rows_all // groups
    cell_block = lambda wide: pl.BlockSpec((group * WW, wide), lambda g: (g, 0))
    return pl.pallas_call(
        lambda *refs: mix_kernel(parts, residual, *refs),
        grid=(groups,),
        in_specs=[
            *[pl.BlockSpec(table.shape, lambda g: (0, 0)) for table in tables],
            *[pl.BlockSpec((owners, rows, chan_part), lambda g: (0, g, 0)) for _ in backs],
            cell_block(channels),
            cell_block(chan_part),
            pl.BlockSpec((out_w.shape[0], out_depth, channels), lambda g: (0, 0, 0)),
        ],
        out_specs=cell_block(channels),
        out_shape=jax.ShapeDtypeStruct((cells, channels), jnp.bfloat16),
        compiler_params=pltpu.CompilerParams(vmem_limit_bytes=56 * 2**20),
        name="mix_and_project",
    )(*tables, *backs, latents, gate, out_w)


def exchange(blocks):
    return lax.all_to_all(blocks, "sp", split_axis=0, concat_axis=0, tiled=True)


def local(latents, spectrum, w_value, w_gate, w_out, embed_table, prompt_ids, noise_step):
    row_count, channels = latents.shape
    chan_part = w_value.shape[1]
    owners = lax.axis_size("sp")
    splits = lax.axis_size("ch")
    lines = row_count // WW
    band = WW // owners
    group = min(lines, max(1, TILE // band))

    parts = 2 if band % 2 == 0 else 1
    sub = band // parts

    table = cas_table(WW).reshape(owners, parts, 1, sub, 1, WW)
    same_line = jnp.eye(group, dtype=jnp.bfloat16).reshape(1, group, 1, group, 1)
    width_tables = [
        (table[:, part] * same_line).reshape(owners * group * sub, group * WW)
        for part in range(parts)
    ]
    height_table = widened(cas_table(HH), sub)
    time_table = widened(cas_table(TT), TILE)
    gains = spectrum.reshape(TT, HH, parts, sub, chan_part)

    full_value = lax.all_gather(w_value, "sp", axis=0)

    full_gate = lax.all_gather(w_gate, "sp", axis=0)
    local_pool = jnp.mean(jnp.take(embed_table, prompt_ids, axis=1).astype(jnp.float32), axis=1)
    offset = lax.axis_index("ch") * chan_part
    depth = w_out.shape[0]
    if splits == 1:
        first = local_pool.astype(jnp.bfloat16)
        rest = local_pool - first.astype(jnp.float32)
        second = rest.astype(jnp.bfloat16)
        third = (rest - second.astype(jnp.float32)).astype(jnp.bfloat16)
        terms = jnp.stack([first, second, third])
        terms = jnp.pad(terms, ((0, TILE - 3), (0, channels - terms.shape[1])))
        full_out = lax.all_gather(jnp.concatenate([w_out, terms], axis=0), "sp", axis=0)
    else:
        pooled_all = lax.all_gather(local_pool, ("sp", "ch"), axis=0, tiled=True)
        pooled = lax.dynamic_slice_in_dim(pooled_all, offset, chan_part)
        rows_out = lax.all_gather(w_out, "sp", axis=0, tiled=True)
        full_out = lax.dynamic_slice_in_dim(rows_out, offset, chan_part, 0)[None]
        depth = chan_part

    planes, backs = [], []
    for part in range(parts):
        sent = width_forward(width_tables[part], latents, owners, lines, sub, group)
        if planes:
            sent, planes[-1], full_value = lax.optimization_barrier((sent, planes[-1], full_value))
        planes.append(exchange(sent))
    for part in range(parts):
        filtered = plane_filter(
            height_table,
            time_table,
            planes[part].reshape(TT * HH * sub, channels),
            full_value,
            gains[:, :, part].reshape(TT, HH * sub, chan_part),
            sub,
        ).reshape(owners, lines * sub, chan_part)
        if backs:
            filtered, backs[-1], full_gate = lax.optimization_barrier(
                (filtered, backs[-1], full_gate)
            )
        elif parts > 1:
            filtered, planes[-1], full_out = lax.optimization_barrier(
                (filtered, planes[-1], full_out)
            )
        backs.append(exchange(filtered))

    if splits == 1:
        pooled = full_out[:, depth : depth + 3, : local_pool.shape[0]].astype(jnp.float32)
        pooled = jnp.sum(pooled, axis=1).reshape(chan_part)
    channel = offset + jnp.arange(chan_part, dtype=jnp.int32)
    modulation = 1.0 + pooled + step_embedding(noise_step, channel, C)

    gate = gate_rows(latents, full_gate, modulation[None, :])
    mixed = mix_and_project(
        [width_table.T for width_table in width_tables],
        backs,
        latents,
        gate,
        full_out,
        depth,
        group,
        splits == 1,
    )
    if splits == 1:
        return mixed
    half_rows = row_count // splits
    summed = lax.psum_scatter(mixed, "ch", scatter_dimension=0, tiled=True).astype(jnp.float32)
    residual = lax.dynamic_slice_in_dim(latents, lax.axis_index("ch") * half_rows, half_rows, 0)
    return (residual.astype(jnp.float32) + summed).astype(jnp.bfloat16)


def solution(mesh):
    placed = (
        P(("grp", "sp"), None),
        P(None, None, "sp", "ch"),
        P("sp", "ch"),
        P("sp", "ch"),
        P("sp", None),
        P(("sp", "ch"), None),
        P("grp"),
        P("grp"),
    )
    return jax.shard_map(
        local, mesh=mesh, in_specs=placed, out_specs=P(("grp", "sp", "ch"), None), check_vma=False
    )
```
